512 devices in a mesh: shift: 2 (over y), blk: 128 (over z, x), depth: 2 (over core).
Axes of the slice: x: 4, y: 2, z: 32, core: 2. Of those that a mesh axis runs over, the one named last changes fastest.
The devices are a block of a 4x8x32 slice.
Arguments:
- density: bfloat16 [512, 32, 128, 128], P(('shift', 'blk')), parts along dimension 0, may hold values from -1.1953125 to 1.1953125
- product_tasks: int32 [3, 256, 4, 128], P(None, ('shift', 'blk')), parts along dimension 1, may hold values from 0 to 64, as said below
Outputs:
- square_blocks: bfloat16 [512, 32, 128, 128], P(('shift', 'blk'), 'depth'), parts along dimension 0
The draws below stay inside these ranges and needn't reach their ends.
There are 2 independent parts, one for each index of `shift`. The reference program is written for one: setup_inputs(seed, part) draws one part's arguments, and reference() takes and returns one part's arrays. A program takes and returns all parts, laid end to end along the dimension named above; each array names one. Nothing has to cross between parts.
Inputs may be any that keep to these rules, and one draw needn't show every extreme that they name: `product_tasks`: for each panel r and offset t the first tasks are exactly the triples in which slot a of panel r holds block (i, j) of P with block row j in panel (r + t) mod 128, slot b of that panel holds block (j, k), and c is the slot of block (i, k) in block row i, where P's block pattern stores 32 distinct block columns in each block row, its own among them; each triple once; the rest are (0, 0, 64). Some panel and offset has exactly 128 triples.
All inputs are finite; a program needn't handle non-finite values.
Results may differ from the reference program's by a relative error of at most 0.001.
Values may be sent and summed in bfloat16 or wider, within the bound.
No kernel may reach another device: no remote copies, remote signals or barrier semaphores. Data moves between devices by JAX's collectives and lax.ppermute only.
A program may use at most 64 MiB of HBM per device.

```python
import jax
import jax.numpy as jnp
from jax import lax

BS = 128
K = 32
RB_DEV = 2
NB = 256
WIN = 4
TASKS = 128
N_BLK = 128


def pattern_columns(key):
    total_rows = RB_DEV * N_BLK
    key_noise, key_pick = jax.random.split(jax.random.fold_in(key, 7))
    noise = jax.random.randint(key_noise, (total_rows, total_rows), 0, 1024)
    places = jnp.arange(total_rows, dtype=jnp.int32)
    distance = jnp.abs(places[None, :] - places[:, None])
    distance = jnp.minimum(distance, total_rows - distance)
    score = distance * 160 + noise
    score = jnp.where(distance == 0, -1, score)
    chosen = jax.random.randint(key_pick, (), 0, N_BLK)
    in_cluster = places // RB_DEV == chosen
    cluster_row = jnp.take(score, chosen * RB_DEV, axis=0)
    cluster_row = jnp.where(in_cluster, -1, cluster_row)
    score = jnp.where(in_cluster[:, None], cluster_row[None, :], score)
    ranked = (score + 1) * total_rows + places[None, :]
    _, columns = lax.top_k(-ranked, K)
    return columns.astype(jnp.int32)


def draw_product_tasks(key, part):
    columns = pattern_columns(key)
    slots = RB_DEV * K
    mine = columns.reshape(N_BLK, slots)
    devices = jnp.arange(N_BLK, dtype=jnp.int32)
    offsets = jnp.arange(WIN, dtype=jnp.int32)
    target_panel = (devices[:, None] + offsets[None, :]) % N_BLK
    in_panel = mine[:, None, :] // RB_DEV == target_panel[:, :, None]
    inner = jnp.arange(K, dtype=jnp.int32)
    second_slot = (mine % RB_DEV)[:, :, None] * K + inner[None, None, :]
    second_column = jnp.take(columns, mine, axis=0)
    row_columns = columns.reshape(N_BLK, RB_DEV, K)
    row_local = jnp.arange(slots, dtype=jnp.int32) // K
    first_columns = row_columns[:, row_local, :]
    match = second_column[:, :, :, None] == first_columns[:, :, None, :]
    found = jnp.any(match, axis=-1)
    where_found = jnp.argmax(match.astype(jnp.int32), axis=-1).astype(jnp.int32)
    result_slot = row_local[None, :, None] * K + where_found
    first_slot = jnp.broadcast_to(jnp.arange(slots, dtype=jnp.int32)[None, :, None], (N_BLK, slots, K))
    valid = in_panel[:, :, :, None] & found[:, None, :, :]
    valid = valid.reshape(N_BLK, WIN, slots * K)
    position = jnp.cumsum(valid.astype(jnp.int32), axis=-1) - 1
    target = jnp.where(valid, position, TASKS)
    dev_index = jnp.broadcast_to(devices[:, None, None], target.shape)
    off_index = jnp.broadcast_to(offsets[None, :, None], target.shape)
    outputs = []
    for source, filler in ((first_slot, 0), (second_slot, 0), (result_slot, slots)):
        values = jnp.broadcast_to(source.reshape(N_BLK, 1, slots * K), target.shape)
        holder = jnp.full((N_BLK, WIN, TASKS + 1), filler, jnp.int32)
        holder = holder.at[dev_index, off_index, target].set(values)
        holder = holder.at[:, :, TASKS].set(filler)
        outputs.append(holder[:, :, :TASKS])
    return jnp.stack(outputs).astype(jnp.int32)


def steps_of(own_key, extent, shards, low, top_value):
    gain = 1.0
    for dim, blocks in shards:
        heights = jax.random.uniform(jax.random.fold_in(jax.random.fold_in(own_key, 6), dim), (blocks,), jnp.float32, low / len(shards), top_value / len(shards))
        gain = gain * jnp.repeat(jnp.exp(heights), extent[dim] // blocks).reshape((-1,) + (1,) * (len(extent) - 1 - dim))
    return gain


def bell_draw(stream_key, dims, width, most, shards=(), kind=jnp.bfloat16):
    loudness = steps_of(stream_key, dims, shards, -0.22, 0.18) if shards else 1.0
    entries = jax.random.normal(stream_key, dims, jnp.float32) * width * loudness
    return jnp.minimum(jnp.maximum(entries, -most), most).astype(kind)


def setup_inputs(seed: int = 0, part: int = 0) -> dict:
    key_of = jax.random.split(jax.random.key(seed), 3)
    part_keys = jax.random.split(jax.random.fold_in(key_of[2], part), 3)
    return {
        "density": bell_draw(part_keys[0], (NB, K, BS, BS), 0.2, 1.1953125, ((0, 128),)),
        "product_tasks": draw_product_tasks(jax.random.fold_in(jax.random.fold_in(key_of[2], part), 71), part),
    }


def reference(density, product_tasks):
    slots = RB_DEV * K
    panels = density.reshape(N_BLK, slots, BS, BS)

    def one_device(index):
        mine = lax.dynamic_index_in_dim(panels, index, 0, keepdims=False)
        total = jnp.zeros((slots + 1, BS, BS), jnp.float32)
        for offset in range(WIN):
            other = (index + offset) % N_BLK
            panel = lax.dynamic_index_in_dim(panels, other.astype(jnp.int32), 0, keepdims=False)
            tasks = lax.dynamic_index_in_dim(product_tasks[:, :, offset], index, 1, keepdims=False)
            first = jnp.take(mine, tasks[0], axis=0).astype(jnp.float32)
            second = jnp.take(panel, tasks[1], axis=0).astype(jnp.float32)
            products = jnp.einsum("nij,njk->nik", first, second)
            total = total + jax.ops.segment_sum(products, tasks[2], num_segments=slots + 1)
        return total[:slots].astype(jnp.bfloat16)

    result = lax.map(one_device, jnp.arange(N_BLK, dtype=jnp.int32))
    return result.reshape(N_BLK * RB_DEV, K, BS, BS)
```

```python
import functools

import jax
import jax.numpy as jnp
from jax import lax
from jax.experimental import pallas as pl
from jax.experimental.pallas import tpu as pltpu
from jax.sharding import PartitionSpec as P


UNROLL = 8
SENDER = 0
WORKER = 1


def move(value, routes):
    layers = lax.axis_size("depth")
    pairs = [(a * layers + b, c * layers + d) for (a, b), (c, d) in routes]
    return lax.ppermute(value, ("blk", "depth"), pairs)


def run_tasks(tasks, offset, groups, mine, panel, total):
    def group(step, carry):
        base = step * UNROLL
        products = []
        for n in range(UNROLL):
            first = mine[tasks[0, offset, base + n]]
            second = panel[tasks[1, offset, base + n]]
            products.append(jnp.dot(first, second, preferred_element_type=jnp.float32))
        for n in range(UNROLL):
            slot = tasks[2, offset, base + n]
            total[slot] = total[slot] + products[n]
        return carry

    lax.fori_loop(0, groups, group, 0)


def begin_kernel(counts, tasks, mine, total):
    def clear(slot, carry):
        total[slot] = jnp.zeros(total.shape[1:], total.dtype)
        return carry

    lax.fori_loop(0, total.shape[0], clear, 0)
    run_tasks(tasks, 0, counts[0], mine, mine, total)


def middle_kernel(offsets, counts, tasks, mine, *refs):
    panels, total = refs[: len(offsets)], refs[-1]
    for place, (offset, panel) in enumerate(zip(offsets, panels)):
        run_tasks(tasks, offset, counts[place], mine, panel, total)


def last_kernel(offsets, counts, tasks, mine, *refs):
    panels, total = refs[: len(offsets)], refs[len(offsets)]
    low, high = refs[-2:]
    for place, (offset, panel) in enumerate(zip(offsets, panels)):
        run_tasks(tasks, offset, counts[place], mine, panel, total)
    rows, half = low.shape[0], low.shape[1]

    @pl.when(counts[len(offsets)] > 0)
    def _():
        for row in range(rows):

            def put(slot, carry):
                low[row, slot] = total[row * 2 * half + slot].astype(low.dtype)
                high[row, slot] = total[row * 2 * half + half + slot].astype(high.dtype)
                return carry

            lax.fori_loop(0, half, put, 0)


SMEM = functools.partial(pl.BlockSpec, memory_space=pltpu.SMEM)
VMEM = functools.partial(pl.BlockSpec, memory_space=pltpu.VMEM)

PARAMS = pltpu.CompilerParams(vmem_limit_bytes=24 * 1024 * 1024)


def cost(blocks, size, tasks):
    return pl.CostEstimate(
        flops=2 * tasks * size**3, bytes_accessed=blocks * size * size * 2, transcendentals=0
    )


def body(density, product_tasks):
    rows, slots, size = density.shape[0], density.shape[1], density.shape[2]
    mine = density.reshape(rows * slots, size, size)
    tasks = product_tasks[:, 0]
    window, places = tasks.shape[1], tasks.shape[2]
    count = lax.axis_size("blk")
    lines = range(count // window)

    def at(line, column):
        return line % len(lines) * window + column

    inner = range(1, window)
    near = [((at(z, x), WORKER), (at(z, x - 1), WORKER)) for z in lines for x in inner]
    far = [((at(z, window - 1), WORKER), (at(z, 0), WORKER)) for z in lines]
    far += [((at(z + 1, x - 1), SENDER), (at(z, x), WORKER)) for z in lines for x in inner]
    ahead = [((at(z, 0), WORKER), (at(z, window - 1), SENDER)) for z in lines]
    across = [((at(z + 1, window - 1), SENDER), (at(z, window - 1), WORKER)) for z in lines]
    up = [((at(z, x - 1), WORKER), (at(z, x), WORKER)) for z in lines for x in inner]
    down = [((at(z, 1), WORKER), (at(z, 0), WORKER)) for z in lines]
    halves = [((p, WORKER), (p, SENDER)) for p in range(count)]

    column = lax.axis_index("blk") % window
    works = lax.axis_index("depth") == WORKER
    groups = jnp.where(works, places // UNROLL, 0).astype(jnp.int32)
    first, final = column == 0, column == window - 1

    moved = move(mine, ahead)
    one = move(mine, near)
    three = move(mine, far)
    crossed = move(moved, across)
    two_up = move(three, up)
    two_down = move(one, down)

    sums = jax.ShapeDtypeStruct((rows * slots + 1, size, size), jnp.float32)
    total = pl.pallas_call(
        begin_kernel,
        out_shape=sums,
        in_specs=[SMEM(), SMEM(), VMEM()],
        out_specs=VMEM(),
        cost_estimate=cost(slots, size, places),
        compiler_params=PARAMS,
        name="begin",
    )(jnp.stack([groups]), tasks, mine)
    counts = jnp.stack([jnp.where(final, 0, groups), groups])
    total = pl.pallas_call(
        functools.partial(middle_kernel, (1, 3)),
        out_shape=sums,
        in_specs=[SMEM(), SMEM(), VMEM(), VMEM(), VMEM(), VMEM()],
        out_specs=VMEM(),
        input_output_aliases={5: 0},
        cost_estimate=cost(slots, size, 2 * places),
        compiler_params=PARAMS,
        name="middle",
    )(counts, tasks, mine, one, three, total)
    counts = jnp.stack(
        [jnp.where(first, 0, groups), jnp.where(first, groups, 0), jnp.where(final, groups, 0), groups]
    )
    half = jax.ShapeDtypeStruct((rows, slots // 2, size, size), jnp.bfloat16)
    low, high = pl.pallas_call(
        functools.partial(last_kernel, (2, 2, 1)),
        out_shape=(half, half),
        in_specs=[SMEM(), SMEM(), VMEM(), VMEM(), VMEM(), VMEM(), VMEM()],
        out_specs=(VMEM(), VMEM()),
        cost_estimate=cost(slots, size, places),
        compiler_params=PARAMS,
        name="last",
    )(counts, tasks, mine, two_up, two_down, crossed, total)
    arrived = move(low, halves)
    return jnp.where(works, high, arrived)


def solution(mesh):
    placed = (P(("shift", "blk"), None, None, None), P(None, ("shift", "blk"), None, None))
    return jax.shard_map(
        body,
        mesh=mesh,
        in_specs=placed,
        out_specs=P(("shift", "blk"), "depth", None, None),
        check_vma=False,
    )
```

```python
import functools

import jax
import jax.numpy as jnp
from jax import lax
from jax.experimental import pallas as pl
from jax.experimental.pallas import tpu as pltpu
from jax.sharding import PartitionSpec as P


UNROLL = 8
SENDER = 0
WORKER = 1


def move(value, routes):
    layers = lax.axis_size("depth")
    pairs = [(a * layers + b, c * layers + d) for (a, b), (c, d) in routes]
    return lax.ppermute(value, ("blk", "depth"), pairs)


def groups_here(tasks):
    column = lax.axis_index("blk") % tasks.shape[1]
    works = lax.axis_index("depth") == WORKER
    groups = jnp.where(works, tasks.shape[2] // UNROLL, 0)
    first, final = column == 0, column == tasks.shape[1] - 1
    return groups, first, final


def run_tasks(tasks, offset, groups, mine, panel, total):
    def group(step, carry):
        base = step * UNROLL
        products = []
        for n in range(UNROLL):
            first = mine[tasks[0, offset, base + n]]
            second = panel[tasks[1, offset, base + n]]
            products.append(jnp.dot(first, second, preferred_element_type=jnp.float32))
        for n in range(UNROLL):
            slot = tasks[2, offset, base + n]
            total[slot] = total[slot] + products[n]
        return carry

    lax.fori_loop(0, groups, group, 0)


def begin_kernel(tasks, mine, total):
    def clear(slot, carry):
        total[slot] = jnp.zeros(total.shape[1:], total.dtype)
        return carry

    works = lax.axis_index("depth") == WORKER
    lax.fori_loop(0, jnp.where(works, total.shape[0], 0), clear, 0)


def load(tasks, plan, arrived):
    copy = pltpu.make_async_copy(tasks, plan, arrived)
    copy.start()
    copy.wait()


def early_kernel(tasks, mine, one, three, before, total, plan, arrived):
    groups, _, final = groups_here(plan)

    @pl.when(groups > 0)
    def _():
        load(tasks, plan, arrived)
        run_tasks(plan, 0, groups, mine, mine, total)
        run_tasks(plan, 1, jnp.where(final, 0, groups), mine, one, total)
        run_tasks(plan, 3, groups, mine, three, total)


def relay_kernel(tasks, mine, up, down, before, total, plan, arrived):
    groups, first, _ = groups_here(plan)

    @pl.when(groups > 0)
    def _():
        load(tasks, plan, arrived)
        run_tasks(plan, 2, jnp.where(first, 0, groups), mine, up, total)
        run_tasks(plan, 2, jnp.where(first, groups, 0), mine, down, total)


def late_kernel(tasks, mine, crossed, total, low, high, plan, arrived):
    groups, _, final = groups_here(plan)

    @pl.when(final & (groups > 0))
    def _():
        load(tasks, plan, arrived)
        run_tasks(plan, 1, groups, mine, crossed, total)

    rows, half = low.shape[0], low.shape[1]
    for row in range(rows):

        def put(slot, carry):
            low[row, slot] = total[row * 2 * half + slot].astype(low.dtype)
            high[row, slot] = total[row * 2 * half + half + slot].astype(high.dtype)
            return carry

        lax.fori_loop(0, jnp.where(groups > 0, half, 0), put, 0)


def finish_kernel(high, sent, result, arrived):
    works = lax.axis_index("depth") == WORKER
    for used, source in ((works, high), (~works, sent)):

        @pl.when(used)
        def _():
            copy = pltpu.make_async_copy(source, result, arrived)
            copy.start()
            copy.wait()


VMEM = functools.partial(pl.BlockSpec, memory_space=pltpu.VMEM)
HBM = functools.partial(pl.BlockSpec, memory_space=pltpu.HBM)


def granted(mib):
    return pltpu.CompilerParams(vmem_limit_bytes=int(mib * 1024 * 1024))


def cost(blocks, size, tasks):
    return pl.CostEstimate(
        flops=2 * tasks * size**3, bytes_accessed=blocks * size * size * 2, transcendentals=0
    )


def body(density, product_tasks):
    rows, slots, size = density.shape[0], density.shape[1], density.shape[2]
    mine = density.reshape(rows * slots, size, size)
    tasks = product_tasks[:, 0]
    window, places = tasks.shape[1], tasks.shape[2]
    count = lax.axis_size("blk")
    lines = range(count // window)

    def at(line, column):
        return line % len(lines) * window + column

    inner = range(1, window)
    near = [((at(z, x), WORKER), (at(z, x - 1), WORKER)) for z in lines for x in inner]
    far = [((at(z, window - 1), WORKER), (at(z, 0), WORKER)) for z in lines]
    far += [((at(z + 1, x - 1), SENDER), (at(z, x), WORKER)) for z in lines for x in inner]
    ahead = [((at(z, 0), WORKER), (at(z, window - 1), SENDER)) for z in lines]
    across = [((at(z + 1, window - 1), SENDER), (at(z, window - 1), WORKER)) for z in lines]
    up = [((at(z, x - 1), WORKER), (at(z, x), WORKER)) for z in lines for x in inner]
    down = [((at(z, 1), WORKER), (at(z, 0), WORKER)) for z in lines]
    halves = [((p, WORKER), (p, SENDER)) for p in range(count)]

    moved = move(mine, ahead)
    one = move(mine, near)
    three = move(mine, far)
    crossed = move(moved, across)
    two_up = move(three, up)
    two_down = move(one, down)

    sums = jax.ShapeDtypeStruct((rows * slots + 1, size, size), jnp.float32)
    half = jax.ShapeDtypeStruct((rows, slots // 2, size, size), jnp.bfloat16)
    scratch = [pltpu.SMEM(tasks.shape, tasks.dtype), pltpu.SemaphoreType.DMA]
    total = pl.pallas_call(
        begin_kernel,
        out_shape=sums,
        in_specs=[HBM(), VMEM()],
        out_specs=VMEM(),
        compiler_params=granted(14),
        name="begin",
    )(tasks, mine)
    total = pl.pallas_call(
        early_kernel,
        out_shape=sums,
        in_specs=[HBM()] + [VMEM()] * 4,
        out_specs=VMEM(),
        input_output_aliases={4: 0},
        scratch_shapes=scratch,
        cost_estimate=cost(3 * slots, size, 3 * places),
        compiler_params=granted(14),
        name="early",
    )(tasks, mine, one, three, total)
    total = pl.pallas_call(
        relay_kernel,
        out_shape=sums,
        in_specs=[HBM()] + [VMEM()] * 4,
        out_specs=VMEM(),
        input_output_aliases={4: 0},
        scratch_shapes=scratch,
        cost_estimate=cost(3 * slots, size, places),
        compiler_params=granted(14),
        name="relay",
    )(tasks, mine, two_up, two_down, total)
    low, high = pl.pallas_call(
        late_kernel,
        out_shape=(half, half),
        in_specs=[HBM()] + [VMEM()] * 3,
        out_specs=(VMEM(), VMEM()),
        scratch_shapes=scratch,
        cost_estimate=cost(2 * slots, size, places),
        compiler_params=granted(14),
        name="late",
    )(tasks, mine, crossed, total)
    arrived = move(low, halves)
    return pl.pallas_call(
        finish_kernel,
        out_shape=half,
        in_specs=[VMEM(), HBM()],
        out_specs=HBM(),
        scratch_shapes=[pltpu.SemaphoreType.DMA],
        compiler_params=granted(14),
        name="finish",
    )(high, arrived)


def solution(mesh):
    placed = (P(("shift", "blk"), None, None, None), P(None, ("shift", "blk"), None, None))
    return jax.shard_map(
        body,
        mesh=mesh,
        in_specs=placed,
        out_specs=P(("shift", "blk"), "depth", None, None),
        check_vma=False,
    )
```

```python
import functools

import jax
import jax.numpy as jnp
from jax import lax
from jax.experimental import pallas as pl
from jax.experimental.pallas import tpu as pltpu
from jax.sharding import PartitionSpec as P


UNROLL = 8
SENDER = 0
WORKER = 1


def move(value, routes):
    layers = lax.axis_size("depth")
    pairs = [(a * layers + b, c * layers + d) for (a, b), (c, d) in routes]
    return lax.ppermute(value, ("blk", "depth"), pairs)


def groups_here(tasks):
    column = lax.axis_index("blk") % tasks.shape[1]
    works = lax.axis_index("depth") == WORKER
    groups = jnp.where(works, tasks.shape[2] // UNROLL, 0)
    first, final = column == 0, column == tasks.shape[1] - 1
    return groups, first, final


def run_tasks(tasks, offset, groups, mine, panel, total):
    def group(step, carry):
        base = step * UNROLL
        products = []
        for n in range(UNROLL):
            first = mine[tasks[0, offset, base + n]]
            second = panel[tasks[1, offset, base + n]]
            products.append(jnp.dot(first, second, preferred_element_type=jnp.float32))
        for n in range(UNROLL):
            slot = tasks[2, offset, base + n]
            total[slot] = total[slot] + products[n]
        return carry

    lax.fori_loop(0, groups, group, 0)


def begin_kernel(tasks, mine, total):
    def clear(slot, carry):
        total[slot] = jnp.zeros(total.shape[1:], total.dtype)
        return carry

    works = lax.axis_index("depth") == WORKER
    lax.fori_loop(0, jnp.where(works, total.shape[0], 0), clear, 0)


def load(tasks, plan, arrived):
    copy = pltpu.make_async_copy(tasks, plan, arrived)
    copy.start()
    copy.wait()


def early_kernel(tasks, mine, one, three, before, total, plan, arrived):
    groups, _, final = groups_here(plan)

    @pl.when(groups > 0)
    def _():
        load(tasks, plan, arrived)
        run_tasks(plan, 0, groups, mine, mine, total)
        run_tasks(plan, 1, jnp.where(final, 0, groups), mine, one, total)
        run_tasks(plan, 3, groups, mine, three, total)


def relay_kernel(tasks, mine, up, down, before, total, plan, arrived):
    groups, first, _ = groups_here(plan)

    @pl.when(groups > 0)
    def _():
        load(tasks, plan, arrived)
        run_tasks(plan, 2, jnp.where(first, 0, groups), mine, up, total)
        run_tasks(plan, 2, jnp.where(first, groups, 0), mine, down, total)


def late_kernel(tasks, mine, crossed, total, low, high, plan, arrived):
    groups, _, final = groups_here(plan)

    @pl.when(final & (groups > 0))
    def _():
        load(tasks, plan, arrived)
        run_tasks(plan, 1, groups, mine, crossed, total)

    rows, half = low.shape[0], low.shape[1]
    for row in range(rows):

        def put(slot, carry):
            low[row, slot] = total[row * 2 * half + slot].astype(low.dtype)
            high[row, slot] = total[row * 2 * half + half + slot].astype(high.dtype)
            return carry

        lax.fori_loop(0, jnp.where(groups > 0, half, 0), put, 0)


def write_kernel(used_by, source, *refs):
    result, arrived = refs[-2:]

    @pl.when(lax.axis_index("depth") == used_by)
    def _():
        copy = pltpu.make_async_copy(source, result, arrived)
        copy.start()
        copy.wait()


VMEM = functools.partial(pl.BlockSpec, memory_space=pltpu.VMEM)
HBM = functools.partial(pl.BlockSpec, memory_space=pltpu.HBM)


def granted(mib):
    return pltpu.CompilerParams(vmem_limit_bytes=int(mib * 1024 * 1024))


def cost(blocks, size, tasks):
    return pl.CostEstimate(
        flops=2 * tasks * size**3, bytes_accessed=blocks * size * size * 2, transcendentals=0
    )


def body(density, product_tasks):
    rows, slots, size = density.shape[0], density.shape[1], density.shape[2]
    mine = density.reshape(rows * slots, size, size)
    tasks = product_tasks[:, 0]
    window, places = tasks.shape[1], tasks.shape[2]
    count = lax.axis_size("blk")
    lines = range(count // window)

    def at(line, column):
        return line % len(lines) * window + column

    inner = range(1, window)
    starts = [WORKER] * (window - 1) + [SENDER]
    near = [((at(z, x), starts[x]), (at(z, x - 1), WORKER)) for z in lines for x in inner]
    far = [((at(z, window - 1), SENDER), (at(z, 0), WORKER)) for z in lines]
    far += [((at(z + 1, x - 1), SENDER), (at(z, x), WORKER)) for z in lines for x in inner]
    ahead = [((at(z, 0), WORKER), (at(z, window - 1), SENDER)) for z in lines]
    across = [((at(z + 1, window - 1), SENDER), (at(z, window - 1), WORKER)) for z in lines]
    up = [((at(z, x - 1), WORKER), (at(z, x), WORKER)) for z in lines for x in inner]
    down = [((at(z, 1), WORKER), (at(z, 0), WORKER)) for z in lines]
    halves = [((p, WORKER), (p, SENDER)) for p in range(count)]

    moved = move(mine, ahead)
    one = move(mine, near)
    three = move(mine, far)
    crossed = move(moved, across)
    two_up = move(three, up)
    two_down = move(one, down)

    sums = jax.ShapeDtypeStruct((rows * slots + 1, size, size), jnp.float32)
    half = jax.ShapeDtypeStruct((rows, slots // 2, size, size), jnp.bfloat16)
    scratch = [pltpu.SMEM(tasks.shape, tasks.dtype), pltpu.SemaphoreType.DMA]
    total = pl.pallas_call(
        begin_kernel,
        out_shape=sums,
        in_specs=[HBM(), VMEM()],
        out_specs=VMEM(),
        compiler_params=granted(14),
        name="begin",
    )(tasks, mine)
    total = pl.pallas_call(
        early_kernel,
        out_shape=sums,
        in_specs=[HBM()] + [VMEM()] * 4,
        out_specs=VMEM(),
        input_output_aliases={4: 0},
        scratch_shapes=scratch,
        cost_estimate=cost(3 * slots, size, 3 * places),
        compiler_params=granted(14),
        name="early",
    )(tasks, mine, one, three, total)
    total = pl.pallas_call(
        relay_kernel,
        out_shape=sums,
        in_specs=[HBM()] + [VMEM()] * 4,
        out_specs=VMEM(),
        input_output_aliases={4: 0},
        scratch_shapes=scratch,
        cost_estimate=cost(3 * slots, size, places),
        compiler_params=granted(14),
        name="relay",
    )(tasks, mine, two_up, two_down, total)
    low, high = pl.pallas_call(
        late_kernel,
        out_shape=(half, half),
        in_specs=[HBM()] + [VMEM()] * 3,
        out_specs=(VMEM(), VMEM()),
        scratch_shapes=scratch,
        cost_estimate=cost(2 * slots, size, places),
        compiler_params=granted(14),
        name="late",
    )(tasks, mine, crossed, total)
    result = pl.pallas_call(
        functools.partial(write_kernel, WORKER),
        out_shape=half,
        in_specs=[VMEM()],
        out_specs=HBM(),
        scratch_shapes=[pltpu.SemaphoreType.DMA],
        compiler_params=granted(14),
        name="own",
    )(high)
    sent = move(low, halves)
    return pl.pallas_call(
        functools.partial(write_kernel, SENDER),
        out_shape=half,
        in_specs=[VMEM(), HBM()],
        out_specs=HBM(),
        input_output_aliases={1: 0},
        scratch_shapes=[pltpu.SemaphoreType.DMA],
        compiler_params=granted(14),
        name="other",
    )(sent, result)


def solution(mesh):
    placed = (P(("shift", "blk"), None, None, None), P(None, ("shift", "blk"), None, None))
    return jax.shard_map(
        body,
        mesh=mesh,
        in_specs=placed,
        out_specs=P(("shift", "blk"), "depth", None, None),
        check_vma=False,
    )
```

```python
import functools

import jax
import jax.numpy as jnp
from jax import lax
from jax.experimental import pallas as pl
from jax.experimental.pallas import tpu as pltpu
from jax.sharding import PartitionSpec as P


SHORT, LONG = 8, 32
SENDER = 0
WORKER = 1


def move(value, routes):
    layers = lax.axis_size("depth")
    pairs = [(a * layers + b, c * layers + d) for (a, b), (c, d) in routes]
    return lax.ppermute(value, ("blk", "depth"), pairs)


def tasks_here(tasks, wraps):
    column = lax.axis_index("blk") % tasks.shape[1]
    last = lax.axis_index("blk") >= lax.axis_size("blk") - tasks.shape[1]
    works = (lax.axis_index("depth") == WORKER) & (last == wraps)
    count = jnp.where(works, tasks.shape[2], 0)
    first, final = column == 0, column == tasks.shape[1] - 1
    return count, first, final


def run_tasks(tasks, offset, count, mine, panel, total, together):
    def step(start, carry):
        for n in range(together):
            place = start * together + n
            slot = tasks[2, offset, place]
            first, second = mine[tasks[0, offset, place]], panel[tasks[1, offset, place]]
            total[slot] = total[slot] + jnp.dot(first, second, preferred_element_type=jnp.float32)
        return carry

    lax.fori_loop(0, count // together, step, 0)


def begin_kernel(total):
    def clear(slot, carry):
        total[slot] = jnp.zeros(total.shape[1:], total.dtype)
        return carry

    works = lax.axis_index("depth") == WORKER
    lax.fori_loop(0, jnp.where(works, total.shape[0], 0), clear, 0)


def load(tasks, plan, arrived):
    copy = pltpu.make_async_copy(tasks, plan, arrived)
    copy.start()
    copy.wait()


def early_kernel(wraps, tasks, mine, one, three, before, total, plan, arrived):
    count, _, final = tasks_here(plan, wraps)

    @pl.when(count > 0)
    def _():
        load(tasks, plan, arrived)
        run_tasks(plan, 0, count, mine, mine, total, SHORT)
        run_tasks(plan, 1, jnp.where(final, 0, count), mine, one, total, SHORT)
        run_tasks(plan, 3, count, mine, three, total, SHORT)


def relay_kernel(wraps, tasks, mine, up, down, before, total, plan, arrived):
    count, first, _ = tasks_here(plan, wraps)

    @pl.when(count > 0)
    def _():
        load(tasks, plan, arrived)
        run_tasks(plan, 2, jnp.where(first, 0, count), mine, up, total, LONG)
        run_tasks(plan, 2, jnp.where(first, count, 0), mine, down, total, LONG)


def late_kernel(wraps, tasks, mine, crossed, total, low, high, plan, arrived):
    count, _, final = tasks_here(plan, wraps)

    @pl.when(final & (count > 0))
    def _():
        load(tasks, plan, arrived)
        run_tasks(plan, 1, count, mine, crossed, total, LONG)

    rows, half = low.shape[0], low.shape[1]
    for row in range(rows):

        def put(slot, carry):
            low[row, slot] = total[row * 2 * half + slot].astype(low.dtype)
            high[row, slot] = total[row * 2 * half + half + slot].astype(high.dtype)
            return carry

        lax.fori_loop(0, jnp.where(count > 0, half, 0), put, 0)


def write_kernel(used_by, wraps, window, source, *refs):
    result, arrived = refs[-2:]

    last = lax.axis_index("blk") >= lax.axis_size("blk") - window

    @pl.when((lax.axis_index("depth") == used_by) & (last == wraps))
    def _():
        rows, half = source.shape[0], source.shape[1]
        part = half // 2
        copies = []
        for n in range(2 * rows):
            place = (n // 2, pl.ds(n % 2 * part, part))
            copies.append(pltpu.make_async_copy(source.at[place], result.at[place], arrived.at[n]))
        for copy in copies:
            copy.start()
        for copy in copies:
            copy.wait()


VMEM = functools.partial(pl.BlockSpec, memory_space=pltpu.VMEM)
HBM = functools.partial(pl.BlockSpec, memory_space=pltpu.HBM)


def granted(mib):
    return pltpu.CompilerParams(vmem_limit_bytes=int(mib * 1024 * 1024))


def cost(blocks, size, tasks):
    return pl.CostEstimate(
        flops=2 * tasks * size**3, bytes_accessed=blocks * size * size * 2, transcendentals=0
    )


def body(density, product_tasks):
    rows, slots, size = density.shape[0], density.shape[1], density.shape[2]
    mine = density.reshape(rows * slots, size, size)
    tasks = product_tasks[:, 0]
    window, places = tasks.shape[1], tasks.shape[2]
    lines = range(lax.axis_size("blk") // window)
    inner = range(1, window)

    def at(line, column):
        return line % len(lines) * window + column

    sides = [WORKER] * (window - 1) + [SENDER]
    left = [((at(z, x), sides[x]), (at(z, (x - 1) % window), sides[x - 1])) for z in lines for x in range(window)]
    sets = (("a", False, lines[:-1]), ("b", True, lines[-1:]))

    sums = jax.ShapeDtypeStruct((rows * slots + 1, size, size), jnp.float32)
    half = jax.ShapeDtypeStruct((rows, slots // 2, size, size), jnp.bfloat16)
    scratch = [pltpu.SMEM(tasks.shape, tasks.dtype), pltpu.SemaphoreType.DMA]

    def kernel(function, out, *operands, in_hbm=(0,), out_spec=VMEM, alias=None, space=scratch, work=1):
        return pl.pallas_call(
            function,
            out_shape=out,
            in_specs=[HBM() if n in in_hbm else VMEM() for n in range(len(operands))],
            out_specs=jax.tree.map(lambda _: out_spec(), out),
            input_output_aliases={} if alias is None else {alias: 0},
            scratch_shapes=space,
            cost_estimate=cost(2 * slots, size, work * places),
            compiler_params=granted(14),
        )(*operands)

    def write(used_by, wraps, source, result):
        return kernel(
            functools.partial(write_kernel, used_by, wraps, window),
            half,
            *((source,) if result is None else (source, result)),
            in_hbm=(1,),
            out_spec=HBM,
            alias=None if result is None else 1,
            space=[pltpu.SemaphoreType.DMA((2 * rows,))],
        )

    three, crossed, down, result = {}, {}, {}, None
    for tag, _, served in reversed(sets):
        routes = [((at(z, window - 1), SENDER), (at(z, 0), WORKER)) for z in served]
        routes += [((at(z + 1, x - 1), SENDER), (at(z, x), WORKER)) for z in served for x in inner]
        three[tag] = move(mine, routes)
    one = move(mine, left)
    for tag, _, served in reversed(sets):
        routes = [((at(z + 1, window - 1), SENDER), (at(z, window - 1), WORKER)) for z in served]
        crossed[tag] = move(one, routes)
        down[tag] = move(one, [((at(z, 1), WORKER), (at(z, 0), WORKER)) for z in served])
    total = kernel(begin_kernel, sums, in_hbm=(), space=[])
    for tag, wraps, served in sets:
        up = move(three[tag], [((at(z, x - 1), WORKER), (at(z, x), WORKER)) for z in served for x in inner])
        total = kernel(
            functools.partial(early_kernel, wraps), sums,
            tasks, mine, one, three[tag], total, alias=4, work=3,
        )
        total = kernel(
            functools.partial(relay_kernel, wraps), sums,
            tasks, mine, up, down[tag], total, alias=4,
        )
        low, high = kernel(
            functools.partial(late_kernel, wraps), (half, half),
            tasks, mine, crossed[tag], total,
        )
        result = write(WORKER, wraps, high, result)
        routes = [((at(z, x), WORKER), (at(z, x), SENDER)) for z in served for x in range(window)]
        sent = move(low, routes)
        result = write(SENDER, wraps, sent, result)
    return result


def solution(mesh):
    placed = (P(("shift", "blk"), None, None, None), P(None, ("shift", "blk"), None, None))
    return jax.shard_map(
        body,
        mesh=mesh,
        in_specs=placed,
        out_specs=P(("shift", "blk"), "depth", None, None),
        check_vma=False,
    )
```
